768 devices in a mesh: dp: 192 (over z, y, core), tensor: 4 (over x).
Axes of the slice: x: 4, y: 8, z: 12, core: 2. Of those that a mesh axis runs over, the one named last changes fastest.
Arguments:
- activations: bfloat16 [49152, 27648], P('dp', 'tensor'), may hold values from -24 to 24
- output_gradient: bfloat16 [49152, 5120], P('dp', 'tensor'), may hold values from -6 to 6
- adapter_a: bfloat16 [4, 6912, 128], P('tensor', 'dp'), may hold values from -0.0390625 to 0.0390625
- adapter_b: bfloat16 [128, 5120], P(None, 'tensor'), may hold values from -0.078125 to 0.078125
- log_ratio: float32 [49152], P('dp'), may hold values from -1.5 to 1.5
- lengths: int32 [3, 16], replicated, may hold values from 1 to 1024, as said below
- rewards: int32 [3, 16], replicated, may hold values from 0 to 10
Outputs:
- grad_a: float32 [4, 6912, 128], P('tensor', 'dp')
- adapter_b_gradient: float32 [128, 5120], P(None, 'tensor')
- loss: float32 [], replicated
The draws below stay inside these ranges and needn't reach their ends.
Inputs may be any that keep to these rules, and one draw needn't show every extreme that they name: `lengths`: in every group some rollout has length 1024.
All inputs are finite; a program needn't handle non-finite values.
Results may differ from the reference program's by a relative error of at most 0.0067.
Values may be sent and summed in bfloat16 or wider, within the bound.
A program may use at most 64 MiB of HBM per device.

```python
import jax
import jax.numpy as jnp
from jax import lax

D = 5120
FF = 27648
R = 128
ROLLOUTS = 16
MOST = 1024
GROUPS = 3
TOKENS = 49152
TP_BLOCKS = 4
FF_TP = 6912


def draw_lengths(key, part):
    first_key, second_key = jax.random.split(jax.random.fold_in(key, 17))
    base = jax.random.randint(first_key, (GROUPS, ROLLOUTS), 1, MOST + 1)
    chosen = jax.random.randint(second_key, (GROUPS, 1), 0, ROLLOUTS)
    column_ids = jnp.arange(ROLLOUTS)[None, :]
    return jnp.where(column_ids == chosen, MOST, base).astype(jnp.int32)


def with_ends(drawn, rng, low, largest):
    shape = drawn.shape
    place = [jax.random.randint(jax.random.fold_in(rng, axis), (), 0, shape[axis]) for axis in range(len(shape))]
    drawn = drawn.at[tuple(place)].set(low)
    longest = shape.index(max(shape))
    place[longest] = (place[longest] + 1) % shape[longest]
    return drawn.at[tuple(place)].set(largest)


def strengthened(result, key, source, target, blocks, factor):
    owner, partner = [(jnp.arange(result.shape[axis_at]) // (result.shape[axis_at] // blocks)).reshape([-1 if axis == axis_at else 1 for axis in range(result.ndim)]) for axis_at in (source, target)]
    chosen = jax.random.permutation(key, blocks)[partner]
    strong = (owner == chosen) | (owner == (partner + blocks // 2) % blocks)
    return jnp.where(strong, factor * result, result)


def levels(stream_key, dims, cuts, low, top_value):
    def one(position, shards_of):
        heights = jax.random.uniform(jax.random.fold_in(jax.random.fold_in(stream_key, 6), position), (shards_of,), jnp.float32, low / len(cuts), top_value / len(cuts))
        return jnp.repeat(jnp.exp(heights), dims[position] // shards_of).reshape((-1,) + (1,) * (len(dims) - position - 1))

    level = one(*cuts[0])
    for cut in cuts[1:]:
        level = level * one(*cut)
    return level


def centred(rng, shape, deviation, limit, cuts=(), kind=jnp.bfloat16):
    level = levels(rng, shape, cuts, -0.22, 0.18) if cuts else 1.0
    values = jax.random.normal(rng, shape, jnp.float32) * deviation * level
    return jnp.minimum(jnp.maximum(values, -limit), limit).astype(kind)


def noise_with(own_key, shape, scale, bound, pieces, heavy, kind=jnp.bfloat16):
    entries = scale * jax.random.normal(own_key, shape, jnp.float32)
    if pieces:
        entries = entries * levels(own_key, shape, pieces, -0.22, 0.18)
    return jnp.clip(strengthened(entries, jax.random.fold_in(own_key, 3), *heavy), -bound, bound).astype(kind)


def setup_inputs(seed: int = 0) -> dict:
    streams_of = jax.random.split(jax.random.key(seed), 8)
    activations = noise_with(streams_of[0], (TOKENS, FF), 1.0, 24.0, ((0, 192), (1, 4)), (0, 1, 192, 6.0))
    output_gradient = centred(streams_of[1], (TOKENS, D), 1.0, 6.0, ((0, 192), (1, 4)))
    adapter_a = centred(streams_of[2], (TP_BLOCKS, FF_TP, R), FF ** -0.5, 0.0390625, ((0, 4), (1, 192)))
    adapter_b = centred(streams_of[3], (R, D), D ** -0.5, 0.078125, ((1, 4),))
    log_ratio = centred(streams_of[4], (TOKENS,), 0.25, 1.5, ((0, 192),), jnp.float32)
    lengths = draw_lengths(jax.random.fold_in(streams_of[7], 71), 0)
    rewards = with_ends(jax.random.randint(streams_of[6], (GROUPS, ROLLOUTS), 0, 11), jax.random.fold_in(streams_of[6], 1), 0, 10).astype(jnp.int32)
    return dict(activations=activations, output_gradient=output_gradient, adapter_a=adapter_a, adapter_b=adapter_b, log_ratio=log_ratio, lengths=lengths, rewards=rewards)


clip_eps = 0.2
adapter_scale_factor = 2.0

def token_terms(length_row, reward_row, log_ratio, offset):
    reward = reward_row.astype(jnp.float32)
    center = jnp.mean(reward)
    spread = jnp.mean((reward - center) * (reward - center))
    advantage = (reward - center) / jnp.sqrt(spread + 1.0)
    ends = jnp.cumsum(length_row).astype(jnp.int32)
    starts = (ends - length_row).astype(jnp.int32)
    slots = jnp.arange(log_ratio.shape[0], dtype=jnp.int32) + offset
    member = ((slots[None, :] >= starts[:, None]) & (slots[None, :] < ends[:, None])).astype(jnp.float32)
    live = lax.optimization_barrier(jnp.sum(member, axis=0))
    token_adv = lax.optimization_barrier(jnp.sum(member * advantage[:, None], axis=0))
    ratio = jnp.exp(log_ratio)
    unclipped = ratio * token_adv
    clipped = jnp.clip(ratio, 1.0 - clip_eps, 1.0 + clip_eps) * token_adv
    token_loss = -jnp.minimum(unclipped, clipped)
    slope = jnp.where(unclipped <= clipped, -unclipped, jnp.zeros_like(unclipped))
    return (live * slope, jnp.sum(live * token_loss), jnp.sum(live))

def reference(activations, output_gradient, adapter_a, adapter_b, log_ratio, lengths, rewards):
    groups = lengths.shape[0]
    offsets = jnp.zeros((groups,), jnp.int32)
    token_coefficient, loss_parts, live_parts = jax.vmap(token_terms)(lengths, rewards, log_ratio.reshape(groups, -1), offsets)
    token_coefficient = token_coefficient.reshape(-1)
    ratio_multiplier = groups / jnp.sum(live_parts)
    a_whole = adapter_a.reshape(-1, adapter_a.shape[2])
    low_rank = jnp.dot(activations, a_whole, preferred_element_type=jnp.float32)
    backward_projection = jnp.dot(output_gradient, adapter_b.T, preferred_element_type=jnp.float32)
    error_rows = (adapter_scale_factor * token_coefficient[:, None] * backward_projection).astype(jnp.bfloat16)
    grad_a = ratio_multiplier * lax.dot_general(activations, error_rows, (((0,), (0,)), ((), ())), preferred_element_type=jnp.float32)
    weighted_error = token_coefficient[:, None] * low_rank
    adapter_b_gradient = ratio_multiplier * adapter_scale_factor * jnp.dot(weighted_error.T, output_gradient.astype(jnp.float32), precision=lax.Precision.HIGHEST)
    loss = ratio_multiplier * jnp.sum(loss_parts)
    return (grad_a.reshape(adapter_a.shape), adapter_b_gradient, loss)
```

```python
import functools

import jax
import jax.numpy as jnp
from jax import lax
from jax.experimental import pallas as pl
from jax.experimental.pallas import tpu as pltpu
from jax.sharding import Mesh
from jax.sharding import PartitionSpec as P

Z, Y, C, X = "dp_0", "dp_1", "dp_2", "tensor"
DP = (Z, Y, C)
BY_AXIS = pl.DeviceIdType.MESH

clip_eps = 0.2
adapter_scale_factor = 2.0
UNIT = 8
LANES = 128


def units_split(total, ny, nz):
    pairs = [
        (a, (total - ny * a) // nz)
        for a in range(1, total // ny + 1)
        if total > ny * a and (total - ny * a) % nz == 0
    ]
    return min(pairs, key=lambda p: abs(ny * p[0] - 0.55 * total))


def far_first(n):
    return sorted(range(1, n), key=lambda k: -min(k, n - k))


def kernel(
    dims,
    act_hbm, og_hbm, b_hbm, a_ref, lr_ref, len_ref, rew_ref,
    ga_ref, gb_ref, loss_ref,
    act, og, bv, coeff_v, back_v, low_v, xb, xl,
    abuf, apart, afull, err_v, pfull, psend, precv, rrecv, rsend, rown, rownb, rmin,
    gbs, usend, urecv, uown, umin, umaj, ufin, ufinp, lmin, lmaj, lcore,
    load_s, xs, xr, as_, ar, aring_s, aring_r, apart_s, apart_r,
    ps, pr, rring_s, rring_r, rmin_s, rmin_r,
    up_s, up_r, um_s, um_r, uj_s, uj_r, uf_s, uf_r, ufp_s, ufp_r,
    lm_s, lm_r, lj_s, lj_r, lc_s, lc_r,
):
    nz, ny, nx, groups, rollouts, rows, blocks, upcs = dims
    z, y, core, x = (lax.axis_index(n) for n in (Z, Y, C, X))
    tokens = act.shape[0]
    zy_all = nz * ny
    per_block = zy_all // blocks
    kb = per_block * 2 * rows
    size = {Z: nz, Y: ny, X: nx}

    def to(axis, index):
        return {axis: index}

    def remote(src, dst, ssem, rsem, axis, index):
        return pltpu.make_async_remote_copy(
            src_ref=src, dst_ref=dst, send_sem=ssem, recv_sem=rsem,
            device_id=to(axis, index), device_id_type=BY_AXIS,
        )

    sent = []

    def start(copy):
        copy.start()
        sent.append(copy)

    barrier = pltpu.get_barrier_semaphore()
    greet = 1
    pl.semaphore_signal(barrier, inc=1, device_id=to(C, 1 - core), device_id_type=BY_AXIS)
    for axis, me in ((Z, z), (Y, y), (X, x)):
        for k in far_first(size[axis]):
            pl.semaphore_signal(
                barrier, inc=1, device_id=to(axis, lax.rem(me + k, size[axis])), device_id_type=BY_AXIS
            )
            greet += 1
    load_og = pltpu.make_async_copy(og_hbm, og, load_s.at[0])
    load_b = pltpu.make_async_copy(b_hbm, bv, load_s.at[1])
    load_act = pltpu.make_async_copy(act_hbm, act, load_s.at[2])
    load_b.start()
    load_og.start()
    load_act.start()

    trows = tokens // LANES
    dpi = (z * ny + y) * 2 + core
    per_group = zy_all * 2 // groups
    g = dpi // per_group
    offset = (dpi % per_group) * tokens
    shape = (trows, LANES)
    slots = (
        lax.broadcasted_iota(jnp.int32, shape, 0) * LANES
        + lax.broadcasted_iota(jnp.int32, shape, 1)
        + offset
    )
    rewards = [jnp.full(shape, rew_ref[g, i], jnp.int32).astype(jnp.float32) for i in range(rollouts)]
    center = sum(rewards[1:], rewards[0]) / rollouts
    spread = sum([(r - center) * (r - center) for r in rewards]) / rollouts
    scale = jnp.sqrt(spread + 1.0)
    live = jnp.zeros(shape, jnp.float32)
    token_adv = jnp.zeros(shape, jnp.float32)
    begin = jnp.zeros(shape, jnp.int32)
    for i in range(rollouts):
        end = begin + jnp.full(shape, len_ref[g, i], jnp.int32)
        member = ((slots >= begin) & (slots < end)).astype(jnp.float32)
        live = live + member
        token_adv = token_adv + member * ((rewards[i] - center) / scale)
        begin = end
    ratio = jnp.exp(lr_ref[...])
    unclipped = ratio * token_adv
    clipped = jnp.clip(ratio, 1.0 - clip_eps, 1.0 + clip_eps) * token_adv
    token_loss = -jnp.minimum(unclipped, clipped)
    slope = jnp.where(unclipped <= clipped, -unclipped, jnp.zeros_like(unclipped))
    coeff = live * slope
    loss_row = jnp.sum(live * token_loss, axis=0, keepdims=True)
    for t in range(trows):
        row = jnp.broadcast_to(coeff[t : t + 1, :], (LANES, LANES))
        coeff_v[t * LANES : (t + 1) * LANES, :] = row.T
    total_len = jnp.zeros((UNIT, LANES), jnp.int32)
    for gi in range(groups):
        for i in range(rollouts):
            total_len = total_len + jnp.full((UNIT, LANES), len_ref[gi, i], jnp.int32)
    factor = groups / total_len.astype(jnp.float32)

    load_b.wait()
    load_og.wait()
    partial_back = lax.dot_general(
        og[...], bv[...], (((1,), (1,)), ((), ())), preferred_element_type=jnp.float32
    )
    xb[x] = partial_back.astype(jnp.bfloat16)
    pl.semaphore_wait(barrier, greet)

    def x_send(buf, base):
        for k in far_first(nx):
            start(remote(buf.at[x], buf.at[x], xs.at[base + k], xr.at[base + k], X, lax.rem(x + k, nx)))

    def x_sum(buf, base):
        for k in range(1, nx):
            src = lax.rem(x - k + nx, nx)
            remote(buf.at[x], buf.at[src], xs.at[base + k], xr.at[base + k], X, src).wait_recv()
        return sum([buf[i].astype(jnp.float32) for i in range(nx)])

    def body(c, maj, min_):
        nmaj, nmin = size[maj], size[min_]
        mj = z if maj == Z else y
        mn = y if maj == Z else z
        hp = nmaj // 2
        hm = nmaj - 1 - hp
        upc = upcs[c]
        oc = 1 - c
        o_nmin = nmaj

        def wrap(i):
            return lax.rem(i + 2 * nmaj, nmaj)

        def zy(d, m):
            return d * ny + m if c == 0 else m * ny + d

        def min_send(src_of, buf, ssem, rsem):
            for k in far_first(nmin):
                t = lax.rem(mn + k, nmin)
                start(remote(src_of(t), buf(mn), ssem.at[k], rsem.at[k], min_, t))

        def min_wait(src_of, buf, ssem, rsem, each=None):
            for k in far_first(nmin)[::-1]:
                f = lax.rem(mn - k + nmin, nmin)
                remote(src_of(f), buf(f), ssem.at[k], rsem.at[k], min_, f).wait_recv()
                if each is not None:
                    each(f)

        def maj_send(src, buf, ssem, rsem):
            for k in far_first(nmaj):
                t = lax.rem(mj + k, nmaj)
                start(remote(src, buf(mj), ssem.at[k], rsem.at[k], maj, t))

        def maj_wait(src, buf, ssem, rsem):
            for k in far_first(nmaj)[::-1]:
                f = lax.rem(mj - k + nmaj, nmaj)
                remote(src, buf(f), ssem.at[k], rsem.at[k], maj, f).wait_recv()

        def a_chunk(d):
            return abuf.at[pl.ds(d * nmin, nmin)]

        def a_first():
            own = mj * nmin + mn
            abuf[own] = a_ref[...]
            min_send(lambda t: a_ref, lambda i: abuf.at[mj * nmin + i], as_, ar)

        def a_first_wait():
            min_wait(lambda t: a_ref, lambda i: abuf.at[mj * nmin + i], as_, ar)

        def a_share(d, slot):
            start(remote(a_chunk(d), apart.at[pl.ds(d * nmin, nmin)], apart_s.at[slot], apart_r.at[slot], C, oc))

        def a_unpack(d):
            for m in range(nmin):
                afull[zy(d, m), c * rows : (c + 1) * rows, :] = abuf[d * nmin + m].astype(jnp.float32)

        def a_ring_send(s):
            if s < hp:
                d = wrap(mj - s)
                start(remote(a_chunk(d), a_chunk(d), aring_s.at[s], aring_r.at[s], maj, wrap(mj + 1)))
            if s < hm:
                d = wrap(mj + s)
                start(remote(a_chunk(d), a_chunk(d), aring_s.at[hp + s], aring_r.at[hp + s], maj, wrap(mj - 1)))

        def a_ring_wait(s):
            if s < hp:
                d = wrap(mj - 1 - s)
                remote(a_chunk(d), a_chunk(d), aring_s.at[s], aring_r.at[s], maj, wrap(mj + 1)).wait_recv()
            if s < hm:
                d = wrap(mj + 1 + s)
                remote(a_chunk(d), a_chunk(d), aring_s.at[hp + s], aring_r.at[hp + s], maj, wrap(mj - 1)).wait_recv()

        def a_ring_use(s):
            if s < hp:
                a_share(wrap(mj - 1 - s), 1 + s)
                a_unpack(wrap(mj - 1 - s))
            if s < hm:
                a_share(wrap(mj + 1 + s), 1 + hp + s)
                a_unpack(wrap(mj + 1 + s))

        def a_partner():
            n2, m2 = nmin, nmaj
            hp2 = n2 // 2
            order = [(0, 0)]
            for s in range(hp2):
                order.append((1 + s, -1 - s))
                if s < n2 - 1 - hp2:
                    order.append((1 + hp2 + s, 1 + s))
            for slot, step in order:
                d = lax.rem(mn + step + 2 * n2, n2)
                part = apart.at[pl.ds(d * m2, m2)]
                remote(part, part, apart_s.at[slot], apart_r.at[slot], C, oc).wait_recv()
                for m in range(m2):
                    at = d * ny + m if oc == 0 else m * ny + d
                    afull[at, oc * rows : (oc + 1) * rows, :] = apart[d * m2 + m].astype(jnp.float32)

        def p_block(j):
            got = lax.dot_general(
                act[:, j * kb : (j + 1) * kb], err_v[...], (((0,), (0,)), ((), ())),
                preferred_element_type=jnp.float32,
            )
            pfull[j * per_block : (j + 1) * per_block] = got.reshape(per_block, 2 * rows, LANES)
            for i in range(j * per_block, (j + 1) * per_block):
                zi, yi = divmod(i, ny)
                at = zi * ny + yi if oc == 0 else yi * nz + zi
                psend[at] = pfull[i, oc * rows : (oc + 1) * rows, :].astype(jnp.bfloat16)

        def p_copy():
            return remote(psend, precv, ps.at[0], pr.at[0], C, oc)

        def r_term(d, m):
            mine = pfull[zy(d, m), c * rows : (c + 1) * rows, :]
            return mine + precv[d * nmin + m].astype(jnp.float32)

        def r_copy(s, plus):
            slot = s if plus else hp + s
            return remote(
                rsend.at[pl.ds(slot * nmin, nmin)], rrecv.at[pl.ds(slot * nmin, nmin)],
                rring_s.at[slot], rring_r.at[slot], maj, wrap(mj + 1) if plus else wrap(mj - 1),
            )

        def r_ring(s):
            for plus, h in ((True, hp), (False, hm)):
                if s >= h:
                    continue
                slot = s if plus else hp + s
                d = wrap(mj + (hp - s)) if plus else wrap(mj - (hm - s))
                if s:
                    r_copy(s - 1, plus).wait_recv()
                for m in range(nmin):
                    v = r_term(d, m)
                    if s:
                        v = v + rrecv[(slot - 1) * nmin + m].astype(jnp.float32)
                    rsend[slot * nmin + m] = v.astype(jnp.bfloat16)
                start(r_copy(s, plus))

        def r_end():
            r_copy(hp - 1, True).wait_recv()
            if hm:
                r_copy(hm - 1, False).wait_recv()
            for m in range(nmin):
                v = r_term(mj, m) + rrecv[(hp - 1) * nmin + m].astype(jnp.float32)
                if hm:
                    v = v + rrecv[(hp + hm - 1) * nmin + m].astype(jnp.float32)
                rown[m] = v
                rownb[m] = v.astype(jnp.bfloat16)
            min_send(lambda t: rownb.at[t], lambda i: rmin.at[i], rmin_s, rmin_r)

        def r_out():
            rmin[mn] = jnp.zeros((rows, LANES), jnp.bfloat16)
            min_wait(lambda t: rownb.at[t], lambda i: rmin.at[i], rmin_s, rmin_r)
            total = rown[mn]
            for m in range(nmin):
                total = total + rmin[m].astype(jnp.float32)
            ga_ref[...] = total * factor[:1, :]

        wide = og.shape[1] // LANES
        first = 0 if c == 0 else ny * upcs[0]
        o_first = 0 if oc == 0 else ny * upcs[0]
        mine_n, other_n = nmin * upc, nmaj * upcs[oc]

        def unit_at(u):
            r, k = divmod(u, wide)
            return slice(r * UNIT, (r + 1) * UNIT), slice(k * LANES, (k + 1) * LANES)

        def u_copy():
            return remote(
                usend.at[pl.ds(0, other_n)], urecv.at[pl.ds(0, other_n)], up_s.at[0], up_r.at[0], C, oc
            )

        def u_from_partner():
            return remote(
                usend.at[pl.ds(0, mine_n)], urecv.at[pl.ds(0, mine_n)], up_s.at[0], up_r.at[0], C, oc
            )

        def u_local():
            low = x_sum(xl, nx)
            weighted = (coeff_v[...] * low).astype(jnp.bfloat16)
            gbs[...] = adapter_scale_factor * lax.dot_general(
                weighted, og[...], (((0,), (0,)), ((), ())), preferred_element_type=jnp.float32
            )
            for j in range(other_n):
                usend[j] = gbs[unit_at(o_first + j)].astype(jnp.bfloat16)
            start(u_copy())

        def u_chunk(ref, i):
            return ref.at[pl.ds(i * upc, upc)]

        def u_scatter():
            u_from_partner().wait_recv()
            for j in range(mine_n):
                v = gbs[unit_at(first + j)] + urecv[j].astype(jnp.float32)
                uown[j] = v.astype(jnp.bfloat16)
            min_send(lambda t: u_chunk(uown, t), lambda i: u_chunk(umin, i), um_s, um_r)

        def u_spread():
            for j in range(upc):
                umin[mn * upc + j] = uown[mn * upc + j]
            min_wait(lambda t: u_chunk(uown, t), lambda i: u_chunk(umin, i), um_s, um_r)
            for j in range(upc):
                v = sum([umin[m * upc + j].astype(jnp.float32) for m in range(nmin)])
                umaj[mj * upc + j] = v.astype(jnp.bfloat16)
            maj_send(u_chunk(umaj, mj), lambda i: u_chunk(umaj, i), uj_s, uj_r)

        def u_share(i, slot):
            start(remote(u_chunk(ufin, i), u_chunk(ufinp, i), ufp_s.at[slot], ufp_r.at[slot], C, oc))

        def u_gather():
            maj_wait(u_chunk(umaj, mj), lambda i: u_chunk(umaj, i), uj_s, uj_r)
            for j in range(upc):
                v = sum([umaj[m * upc + j].astype(jnp.float32) for m in range(nmaj)])
                ufin[mn * upc + j] = v.astype(jnp.bfloat16)
            min_send(lambda t: u_chunk(ufin, mn), lambda i: u_chunk(ufin, i), uf_s, uf_r)
            u_share(mn, 0)

        def u_out():
            for k in far_first(nmin)[::-1]:
                f = lax.rem(mn - k + nmin, nmin)
                remote(u_chunk(ufin, mn), u_chunk(ufin, f), uf_s.at[k], uf_r.at[k], min_, f).wait_recv()
                u_share(f, k)
            for j in range(mine_n):
                gb_ref[unit_at(first + j)] = ufin[j].astype(jnp.float32) * factor
            o_upc, n2 = upcs[oc], nmaj
            for k in [0] + far_first(n2)[::-1]:
                f = lax.rem(mj - k + n2, n2)
                part = ufinp.at[pl.ds(f * o_upc, o_upc)]
                remote(part, part, ufp_s.at[k], ufp_r.at[k], C, oc).wait_recv()
            for j in range(other_n):
                gb_ref[unit_at(o_first + j)] = ufinp[j].astype(jnp.float32) * factor

        def l_first():
            lmin[mn] = jnp.broadcast_to(loss_row, (UNIT, LANES))
            min_send(lambda t: lmin.at[mn], lambda i: lmin.at[i], lm_s, lm_r)

        def l_second():
            min_wait(lambda t: lmin.at[mn], lambda i: lmin.at[i], lm_s, lm_r)
            lmaj[mj] = sum([lmin[m] for m in range(nmin)])
            maj_send(lmaj.at[mj], lambda i: lmaj.at[i], lj_s, lj_r)

        def l_core():
            return remote(lcore.at[c], lcore.at[c], lc_s.at[0], lc_r.at[0], C, oc)

        def l_third():
            maj_wait(lmaj.at[mj], lambda i: lmaj.at[i], lj_s, lj_r)
            lcore[c] = sum([lmaj[m] for m in range(nmaj)])
            start(l_core())

        def l_out():
            remote(lcore.at[oc], lcore.at[oc], lc_s.at[0], lc_r.at[0], C, oc).wait_recv()
            total = jnp.sum(lcore[0] + lcore[1], axis=1, keepdims=True)
            loss_ref[...] = jnp.broadcast_to(total, (UNIT, LANES)) * factor

        a_first()
        x_send(xb, 0)
        l_first()
        back = x_sum(xb, 0)
        err_v[...] = ((adapter_scale_factor * coeff_v[...]) * back).astype(jnp.bfloat16)
        a_first_wait()
        a_ring_send(0)
        a_share(mj, 0)
        a_unpack(mj)
        load_act.wait()
        done = 0
        for s in range(hp):
            want = -(-blocks * (s + 1) // hp)
            while done < min(want, blocks):
                p_block(done)
                done += 1
            if s == 0:
                l_second()
            a_ring_wait(s)
            a_ring_send(s + 1)
            a_ring_use(s)
        start(p_copy())
        a_partner()
        low = jnp.zeros((tokens, LANES), jnp.float32)
        for j in range(blocks):
            part = afull[j * per_block : (j + 1) * per_block].reshape(kb, LANES).astype(jnp.bfloat16)
            low = low + jnp.dot(act[:, j * kb : (j + 1) * kb], part, preferred_element_type=jnp.float32)
        xl[x] = low.astype(jnp.bfloat16)
        x_send(xl, nx)
        l_third()
        p_copy().wait_recv()
        r_ring(0)
        r_ring(1)
        u_local()
        steps = [functools.partial(r_ring, s) for s in range(2, hp)]
        for f in steps[:1]:
            f()
        u_scatter()
        for f in steps[1:]:
            f()
        u_spread()
        r_end()
        l_out()
        u_gather()
        r_out()
        u_out()

    @pl.when(core == 0)
    def _():
        mark = len(sent)
        body(0, Z, Y)
        for copy in sent[mark:]:
            copy.wait_send()
        del sent[mark:]

    @pl.when(core == 1)
    def _():
        mark = len(sent)
        body(1, Y, Z)
        for copy in sent[mark:]:
            copy.wait_send()
        del sent[mark:]


def local(dims, activations, output_gradient, adapter_a, adapter_b, log_ratio, lengths, rewards):
    nz, ny, nx, groups, rollouts, rows, blocks, upcs = dims
    tokens, k = activations.shape
    width = output_gradient.shape[1]
    rank = adapter_b.shape[0]
    n = max(nz, ny)
    zy = nz * ny
    most = max(ny * upcs[0], nz * upcs[1])
    most_maj = max(nz * upcs[0], ny * upcs[1])
    most_other = most
    bf, f32 = jnp.bfloat16, jnp.float32
    vm, dma = pltpu.VMEM, pltpu.SemaphoreType.DMA
    ga, gb, loss = pl.pallas_call(
        functools.partial(kernel, dims),
        out_shape=(
            jax.ShapeDtypeStruct((rows, rank), f32),
            jax.ShapeDtypeStruct((rank, width), f32),
            jax.ShapeDtypeStruct((UNIT, LANES), f32),
        ),
        in_specs=[pl.BlockSpec(memory_space=pl.ANY)] * 3
        + [pl.BlockSpec(memory_space=pltpu.VMEM)] * 2
        + [pl.BlockSpec(memory_space=pltpu.SMEM)] * 2,
        out_specs=tuple([pl.BlockSpec(memory_space=pltpu.VMEM)] * 3),
        scratch_shapes=[
            vm((tokens, k), bf), vm((tokens, width), bf), vm((rank, width), bf),
            vm((tokens, rank), f32), vm((tokens, rank), f32), vm((tokens, rank), f32),
            vm((nx, tokens, rank), bf), vm((nx, tokens, rank), bf),
            vm((zy, rows, rank), bf), vm((zy, rows, rank), bf), vm((zy, 2 * rows, rank), f32),
            vm((tokens, rank), bf), vm((zy, 2 * rows, rank), f32),
            vm((zy, rows, rank), bf), vm((zy, rows, rank), bf),
            vm((zy, rows, rank), bf), vm((zy, rows, rank), bf),
            vm((n, rows, rank), f32), vm((n, rows, rank), bf), vm((n, rows, rank), bf),
            vm((rank, width), f32),
            vm((most_other, UNIT, LANES), bf), vm((most, UNIT, LANES), bf), vm((most, UNIT, LANES), bf),
            vm((most, UNIT, LANES), bf), vm((most_maj, UNIT, LANES), bf),
            vm((most, UNIT, LANES), bf), vm((most, UNIT, LANES), bf),
            vm((n, UNIT, LANES), f32), vm((n, UNIT, LANES), f32), vm((2, UNIT, LANES), f32),
            dma((3,)), dma((2 * nx,)), dma((2 * nx,)), dma((n,)), dma((n,)),
            dma((n,)), dma((n,)), dma((n,)), dma((n,)),
            dma((1,)), dma((1,)), dma((n,)), dma((n,)), dma((n,)), dma((n,)),
            dma((1,)), dma((1,)), dma((n,)), dma((n,)), dma((n,)), dma((n,)),
            dma((n,)), dma((n,)), dma((n,)), dma((n,)),
            dma((n,)), dma((n,)), dma((n,)), dma((n,)), dma((1,)), dma((1,)),
        ],
        compiler_params=pltpu.CompilerParams(
            collective_id=0, has_side_effects=True, vmem_limit_bytes=56 * 1024 * 1024
        ),
        name="grpo",
    )(
        activations, output_gradient, adapter_b, adapter_a[0],
        log_ratio.reshape(tokens // LANES, LANES), lengths, rewards,
    )
    return ga[None], gb, loss[0, 0]


def dims_of(mesh_shape, k, width, rank, groups, rollouts):
    nz, ny, nx = mesh_shape
    rows = k // (nz * ny * 2)
    zy = nz * ny
    blocks = next(
        (zy // b for b in range(16, zy + 1) if zy % b == 0 and (b * 2 * rows) % LANES == 0), 1
    )
    upcs = units_split((rank // UNIT) * (width // LANES), ny, nz)
    return (nz, ny, nx, groups, rollouts, rows, blocks, upcs)


def solution_of(mesh, nz, ny):
    nx = mesh.shape["tensor"]
    split = Mesh(mesh.devices.reshape(nz, ny, 2, nx), (Z, Y, C, X))

    def step(activations, output_gradient, adapter_a, adapter_b, log_ratio, lengths, rewards):
        dims = dims_of(
            (nz, ny, nx), activations.shape[1] // nx, output_gradient.shape[1] // nx,
            adapter_b.shape[0], *lengths.shape,
        )
        return jax.shard_map(
            functools.partial(local, dims),
            mesh=split,
            in_specs=(P(DP, X), P(DP, X), P(X, DP, None), P(None, X), P(DP), P(), P()),
            out_specs=(P(X, DP, None), P(None, X), P()),
            check_vma=False,
        )(activations, output_gradient, adapter_a, adapter_b, log_ratio, lengths, rewards)

    return step


def solution(mesh):
    return solution_of(mesh, 12, 8)
```
